32 devices in a mesh: gy: 16 (over z, x, core), gz: 2 (over y).
Axes of the slice: x: 2, y: 2, z: 4, core: 2. Of those that a mesh axis runs over, the one named last changes fastest.
Arguments:
- populations: float32 [19, 4, 128, 2048], P(None, None, 'gy', 'gz'), may hold values from 0 to 1, as said below
- solid_mask: int32 [4, 128, 2048], P(None, 'gy', 'gz'), may hold values 0 or 1
- body_force: float32 [3], replicated, may hold values from 0.002 to 0.008
Outputs:
- density: float32 [4, 128, 2048], P(None, 'gy', 'gz')
- velocity: float32 [3, 4, 128, 2048], P(None, None, 'gy', 'gz')
The draws below stay inside these ranges and needn't reach their ends.
Inputs may be any that keep to these rules, and one draw needn't show every extreme that they name: `populations`: every population is positive, near its lattice weight times one.
All inputs are finite; a program needn't handle non-finite values. No bound on the sum of `solid_mask` on one device may be relied on, other than what follows from the above.
Results may differ from the reference program's by a relative error of at most 0.0003.
Values sent between devices are 32-bit elements; how exact they have to be, the bound alone decides.
A program may use at most 64 MiB of HBM per device.

```python
import jax
import jax.numpy as jnp
from jax import lax

PLANES = 4
STEPS = 3
NY = 128
NZ = 2048


def draw_populations(key, part):
    weight_list = [1.0 / 3.0] + [1.0 / 18.0] * 6 + [1.0 / 36.0] * 12
    lift_list = [0, 0, 0, 0, 0, 1, -1, 0, 0, 0, 0, 1, -1, -1, 1, 1, -1, -1, 1]
    wfull = jnp.asarray(weight_list, dtype=jnp.float32).reshape(19, 1, 1, 1)
    lift = jnp.asarray(lift_list, dtype=jnp.float32).reshape(19, 1, 1, 1)
    shape = (19, PLANES, NY, NZ)
    rough = 1.0 + jax.random.uniform(key, shape, jnp.float32, -0.4, 0.4)
    return wfull * rough * (1.0 + 0.09 * lift)


def with_ends(values, key, least, top_value):
    longest = values.shape.index(max(values.shape))
    spots = []
    for shift in (0, 1):
        where = [jax.random.randint(jax.random.fold_in(key, axis), (), 0, length) for axis, length in enumerate(values.shape)]
        where[longest] = (where[longest] + shift) % values.shape[longest]
        spots.append(tuple(where))
    return values.at[spots[0]].set(least).at[spots[1]].set(top_value)


def setup_inputs(seed: int = 0) -> dict:
    streams_of = jax.random.split(jax.random.key(seed), 4)
    return {
        "populations": draw_populations(jax.random.fold_in(streams_of[3], 71), 0),
        "solid_mask": with_ends((jax.random.randint(streams_of[1], (PLANES, NY, NZ), 0, 4) < 1).astype(jnp.int32), jax.random.fold_in(streams_of[1], 1), 0, 1),
        "body_force": jnp.clip(jax.random.uniform(streams_of[2], (3,), jnp.float32, 0.002, 0.008), 0.002, 0.008),
    }


velocities = [(0, 0, 0), (1, 0, 0), (-1, 0, 0), (0, 1, 0), (0, -1, 0), (0, 0, 1), (0, 0, -1),
              (1, 1, 0), (-1, -1, 0), (1, -1, 0), (-1, 1, 0), (1, 0, 1), (-1, 0, -1),
              (1, 0, -1), (-1, 0, 1), (0, 1, 1), (0, -1, -1), (0, 1, -1), (0, -1, 1)]
opposite = [0, 2, 1, 4, 3, 6, 5, 8, 7, 10, 9, 12, 11, 14, 13, 16, 15, 18, 17]
lattice_weights = [1.0 / 3.0] + [1.0 / 18.0] * 6 + [1.0 / 36.0] * 12
reference_mach = 0.05


def invert_list(matrix):
    count = len(matrix)
    work = [list(matrix[i]) + [1.0 if i == j else 0.0 for j in range(count)] for i in range(count)]
    for column in range(count):
        pivot = column
        for row in range(column + 1, count):
            if abs(work[row][column]) > abs(work[pivot][column]):
                pivot = row
        work[column], work[pivot] = work[pivot], work[column]
        factor = work[column][column]
        work[column] = [entry / factor for entry in work[column]]
        for row in range(count):
            if row != column:
                scale = work[row][column]
                if scale != 0.0:
                    work[row] = [a - scale * b for a, b in zip(work[row], work[column])]
    return [line[count:] for line in work]


def relax_table():
    columns = []
    for shift_x, shift_y, shift_z in velocities:
        columns.append([1, shift_x, shift_y, shift_z, shift_x ** 2, shift_y ** 2, shift_z ** 2,
                        shift_x * shift_y, shift_x * shift_z, shift_y * shift_z,
                        shift_x ** 2 * shift_y, shift_x ** 2 * shift_z, shift_y ** 2 * shift_x,
                        shift_y ** 2 * shift_z, shift_z ** 2 * shift_x, shift_z ** 2 * shift_y,
                        shift_x ** 2 * shift_y ** 2, shift_x ** 2 * shift_z ** 2, shift_y ** 2 * shift_z ** 2])
    moments = [[float(columns[k][a]) for k in range(19)] for a in range(19)]
    inverse = invert_list(moments)
    rates = [0.0] * 4 + [1.25] * 6 + [1.6] * 6 + [1.3] * 3
    table = [[sum(inverse[i][a] * rates[a] * moments[a][j] for a in range(19)) for j in range(19)]
             for i in range(19)]
    return jnp.asarray(table, dtype=jnp.float32)


def collide(current, body_force, relax):
    cvec = jnp.asarray(velocities, dtype=jnp.float32)
    wvec = jnp.asarray(lattice_weights, dtype=jnp.float32)
    wfull = wvec.reshape(19, 1, 1, 1)
    density = jnp.sum(current, axis=0)
    momentum = jnp.tensordot(cvec.T, current, axes=1, precision=lax.Precision.HIGHEST)
    flow = momentum / density
    projected = jnp.tensordot(cvec, flow, axes=1, precision=lax.Precision.HIGHEST)
    speed_sq = jnp.sum(flow * flow, axis=0)
    equilibrium = wfull * density * (1.0 + 3.0 * projected + 4.5 * projected * projected - 1.5 * speed_sq)
    departure = (current - equilibrium).reshape(19, -1)
    change = jnp.dot(relax, departure, precision=lax.Precision.HIGHEST).reshape(current.shape)
    forcing = 3.0 * wvec * jnp.dot(cvec, body_force, precision=lax.Precision.HIGHEST)
    return current - change + forcing.reshape(19, 1, 1, 1)


def stream(padded, solid_pad, center):
    planes, across, length = center.shape[1:]
    result = []
    for k in range(19):
        shift_x, shift_y, shift_z = velocities[k]
        source = padded[k, 1 - shift_x:1 - shift_x + planes, 1 - shift_y:1 - shift_y + across,
                        1 - shift_z:1 - shift_z + length]
        blocked = solid_pad[1 - shift_x:1 - shift_x + planes, 1 - shift_y:1 - shift_y + across,
                            1 - shift_z:1 - shift_z + length]
        result.append(jnp.where(blocked > 0, center[opposite[k]], source))
    return jnp.stack(result)


def moments_out(current, solid_core):
    cvec = jnp.asarray(velocities, dtype=jnp.float32)
    fluid = (1 - solid_core).astype(jnp.float32)
    density = jnp.sum(current, axis=0)
    momentum = jnp.tensordot(cvec.T, current, axes=1, precision=lax.Precision.HIGHEST)
    return density * fluid, momentum / density / reference_mach * fluid


def reference(populations, solid_mask, body_force):
    relax = relax_table()
    solid_pad = jnp.pad(solid_mask, ((0, 0), (1, 1), (1, 1)), mode="wrap")
    solid_pad = jnp.pad(solid_pad, ((1, 1), (0, 0), (0, 0)), constant_values=1)
    current = populations
    for sweep in range(STEPS):
        relaxed = collide(current, body_force, relax)
        padded = jnp.pad(relaxed, ((0, 0), (0, 0), (1, 1), (1, 1)), mode="wrap")
        padded = jnp.pad(padded, ((0, 0), (1, 1), (0, 0), (0, 0)))
        current = stream(padded, solid_pad, relaxed)
    return moments_out(current, solid_mask)
```

```python
import functools

import jax
import jax.numpy as jnp
from jax import lax
from jax.experimental import pallas as pl
from jax.experimental.pallas import tpu as pltpu
from jax.sharding import PartitionSpec as P

STEPS = 3
W = 128

velocities = [
    (0, 0, 0),
    (1, 0, 0),
    (-1, 0, 0),
    (0, 1, 0),
    (0, -1, 0),
    (0, 0, 1),
    (0, 0, -1),
    (1, 1, 0),
    (-1, -1, 0),
    (1, -1, 0),
    (-1, 1, 0),
    (1, 0, 1),
    (-1, 0, -1),
    (1, 0, -1),
    (-1, 0, 1),
    (0, 1, 1),
    (0, -1, -1),
    (0, 1, -1),
    (0, -1, 1),
]
opposite = [0, 2, 1, 4, 3, 6, 5, 8, 7, 10, 9, 12, 11, 14, 13, 16, 15, 18, 17]
reference_mach = 0.05
Y_SET = {s: [k for k in range(19) if velocities[k][1] == s] for s in (1, -1)}
Z_SET = {s: [k for k in range(19) if velocities[k][2] == s] for s in (1, -1)}
ROUTES = [(1, 0), (-1, 0), (0, 1), (0, -1), (1, 1), (-1, 1), (1, -1), (-1, -1)]


def moments(f):
    s = [f[2 * a + 1] + f[2 * a + 2] for a in range(9)]
    d = [f[2 * a + 1] - f[2 * a + 2] for a in range(9)]
    axy, axz, ayz = s[3] + s[4], s[5] + s[6], s[7] + s[8]
    bxy, bxz, byz = s[3] - s[4], s[5] - s[6], s[7] - s[8]
    pxy, pxz, pyz = d[3] + d[4], d[5] + d[6], d[7] + d[8]
    qxy, qxz, qyz = d[3] - d[4], d[5] - d[6], d[7] - d[8]
    rho = (f[0] + s[0]) + (s[1] + s[2]) + ((axy + axz) + ayz)
    jx = d[0] + (pxy + pxz)
    jy = d[1] + (qxy + pyz)
    jz = d[2] + (qxz + qyz)
    return s, (axy, axz, ayz), (bxy, bxz, byz), (pxy, pxz, pyz), (qxy, qxz, qyz), rho, jx, jy, jz


def collide(f, force):
    s, (axy, axz, ayz), (bxy, bxz, byz), (pxy, pxz, pyz), (qxy, qxz, qyz), rho, jx, jy, jz = moments(f)
    inv = 1.0 / rho
    ux, uy, uz = jx * inv, jy * inv, jz * inv
    rxx, ryy, rzz = jx * ux, jy * uy, jz * uz
    third, ninth = rho * (1.0 / 3.0), rho * (1.0 / 9.0)
    e = 0.625
    exx = e * (s[0] + axy + axz - third - rxx)
    eyy = e * (s[1] + axy + ayz - third - ryy)
    ezz = e * (s[2] + axz + ayz - third - rzz)
    gxy = 0.5 * e * (bxy - jx * uy)
    gxz = 0.5 * e * (bxz - jx * uz)
    gyz = 0.5 * e * (byz - jy * uz)
    sq = (rxx + ryy + rzz) * (1.0 / 3.0)
    h = 0.65
    base = ninth + sq
    hxy = h * (axy - base + 0.5 * rzz)
    hxz = h * (axz - base + 0.5 * ryy)
    hyz = h * (ayz - base + 0.5 * rxx)
    t = 0.8
    jx3, jy3, jz3 = jx * (1.0 / 3.0), jy * (1.0 / 3.0), jz * (1.0 / 3.0)
    tpxy, tpxz, tpyz = t * (pxy - jx3), t * (pxz - jx3), t * (pyz - jy3)
    tqxy, tqxz, tqyz = t * (qxy - jy3), t * (qxz - jz3), t * (qyz - jz3)
    fx, fy, fz = force
    axis_w, edge_w = 3.0 / 18.0, 3.0 / 36.0
    even = [exx - hxy - hxz, eyy - hxy - hyz, ezz - hxz - hyz]
    odd = [-(tpxy + tpxz) - axis_w * fx, -(tqxy + tpyz) - axis_w * fy, -(tqxz + tqyz) - axis_w * fz]
    edges = (
        (hxy, gxy, tpxy, tqxy, fx, fy),
        (hxz, gxz, tpxz, tqxz, fx, fz),
        (hyz, gyz, tpyz, tqyz, fy, fz),
    )
    for hh, gg, tp, tq, fa, fb in edges:
        even += [0.5 * hh + gg, 0.5 * hh - gg]
        odd += [0.5 * (tp + tq) - edge_w * (fa + fb), 0.5 * (tp - tq) - edge_w * (fa - fb)]
    out = [f[0] + 2.0 * ((exx + eyy + ezz) - (hxy + hxz + hyz))]
    for a in range(9):
        out.append(f[2 * a + 1] - even[a] - odd[a])
        out.append(f[2 * a + 2] - even[a] + odd[a])
    return out


def kernel(gy, gz, pop_hbm, mask_hbm, force_ref, den_ref, vel_ref, raw, mask, bits, cells, ys, yh, zs, zh,
           mys, myh, mzs, mzh, load_sem, send_sem, recv_sem):
    planes, across, length = mask_hbm.shape
    chunks = length // W
    my, mz = lax.axis_index("gy"), lax.axis_index("gz")

    def peer(dy, dz):
        return {"gy": lax.rem(my + dy + gy, gy), "gz": lax.rem(mz + dz + gz, gz)}

    load_mask = pltpu.make_async_copy(mask_hbm, mask.at[:, :, W : W + length], load_sem.at[0])
    load_pop = pltpu.make_async_copy(pop_hbm, raw, load_sem.at[1])
    load_mask.start()
    load_pop.start()
    barrier = pltpu.get_barrier_semaphore()
    for dy, dz in ROUTES:
        pl.semaphore_signal(barrier, inc=1, device_id=peer(dy, dz), device_id_type=pl.DeviceIdType.MESH)

    lane = lax.broadcasted_iota(jnp.int32, (across, W), 1)
    sub = lax.broadcasted_iota(jnp.int32, (across, W), 0)
    edge_row = {1: across - 1, -1: 0}

    def copies(number, rows_out, rows_in, packed_out, packed_in):
        result = []
        for i, (dy, dz) in enumerate(ROUTES):
            if dz == 0:
                side = (1 - dy) // 2
                source, target = rows_out.at[side], rows_in.at[side, :, W : W + length]
            else:
                source, target = packed_out.at[(1 - dz) // 2], packed_in.at[i - 2]
            result.append(
                pltpu.make_async_remote_copy(
                    src_ref=source,
                    dst_ref=target,
                    send_sem=send_sem.at[number, i],
                    recv_sem=recv_sem.at[number, i],
                    device_id=peer(dy, dz),
                    device_id_type=pl.DeviceIdType.MESH,
                )
            )
        return result

    def pack_columns(items, first, zero):
        packed = zero
        for j, block in enumerate(items):
            shift = (j if first else j + 1) % W
            moved = pltpu.roll(block, shift, 1) if shift else block
            packed = jnp.where(lane == j, moved, packed)
        return packed

    def unpack(block, j, last):
        shift = (W - 1 - j if last else W - j) % W
        return pltpu.roll(block, shift, 1) if shift else block

    def pull(cell, row, c, base):
        cy, cz = c[1], c[2]

        def at(offset):
            v = cell(offset)
            if cy:
                v = jnp.where(sub == edge_row[cy], row(offset), v)
            return v

        v = at(base)
        if cz == 1:
            v = pltpu.roll(jnp.where(lane == W - 1, at(base - W), v), 1, 1)
        elif cz == -1:
            v = pltpu.roll(jnp.where(lane == 0, at(base + W), v), W - 1, 1)
        if cy:
            v = pltpu.roll(v, 1 if cy == 1 else across - 1, 0)
        return v

    load_mask.wait()
    for side, sign in enumerate((1, -1)):
        for p in range(planes):
            r = edge_row[sign]
            mys[side, p : p + 1, :] = mask[p, r : r + 1, W : W + length]
        offset = length if sign == 1 else W
        mzs[side] = pack_columns(
            [mask[p, :, offset : offset + W] for p in range(planes)], sign == -1, jnp.zeros((across, W), jnp.int32)
        )
    pl.semaphore_wait(barrier, len(ROUTES))
    mask_copies = copies(0, mys, myh, mzs, mzh)
    for copy in mask_copies:
        copy.start()

    force = (force_ref[0], force_ref[1], force_ref[2])

    def relax_and_store(step, f, p, base, into):
        relaxed = collide(f, force)
        for k in range(19):
            cells[into, k, p, :, pl.ds(base, W)] = relaxed[k]
        start = pl.multiple_of(base - W, W)
        for side, sign in enumerate((1, -1)):
            r = edge_row[sign]
            for i, k in enumerate(Y_SET[sign]):
                j = i * planes + p
                ys[step, side, j : j + 1, pl.ds(start, W)] = relaxed[k][r : r + 1, :]

    def send(step, into):
        for side, sign in enumerate((1, -1)):
            offset = length if sign == 1 else W
            zs[step, side] = pack_columns(
                [cells[into, k, p, :, offset : offset + W] for k in Z_SET[sign] for p in range(planes)],
                sign == -1,
                jnp.zeros((across, W), jnp.float32),
            )
        out = copies(1 + step, ys.at[step], yh.at[step], zs.at[step], zh.at[step])
        for copy in out:
            copy.start()
        return out

    def arrive(step, into, out):
        for copy in out:
            copy.wait_recv()
        for zside, zsign in enumerate((1, -1)):
            offset = 0 if zsign == 1 else W + length
            block = zh[step, ROUTES.index((0, zsign)) - 2]
            for i, k in enumerate(Z_SET[zsign]):
                for p in range(planes):
                    cells[into, k, p, :, offset : offset + W] = unpack(block, i * planes + p, zsign == 1)
            for yside, ysign in enumerate((1, -1)):
                corner = zh[step, ROUTES.index((ysign, zsign)) - 2]
                r = edge_row[ysign]
                k = velocities.index((0, ysign, zsign))
                for p in range(planes):
                    moved = unpack(corner, Z_SET[zsign].index(k) * planes + p, zsign == 1)
                    j = Y_SET[ysign].index(k) * planes + p
                    yh[step, yside, j : j + 1, offset : offset + W] = moved[r : r + 1, :]

    def streamed(step, into, p, base):
        flags = bits[p, :, pl.ds(pl.multiple_of(base - W, W), W)]
        f = []
        for k in range(19):
            c = velocities[k]
            here = cells[into, opposite[k], p, :, pl.ds(base, W)]
            q = p - c[0]
            if k == 0:
                moved = here
            elif q < 0 or q >= planes:
                f.append(here)
                continue
            else:

                def cell(offset, k=k, q=q):
                    return cells[into, k, q, :, pl.ds(pl.multiple_of(offset, W), W)]

                def row(offset, k=k, q=q, c=c):
                    j = Y_SET[c[1]].index(k) * planes + q
                    return yh[step, (1 - c[1]) // 2, j : j + 1, pl.ds(pl.multiple_of(offset, W), W)]

                moved = pull(cell, row, c, base)
            f.append(moved if k == 0 else jnp.where((flags & (1 << k)) != 0, here, moved))
        return f

    load_pop.wait()

    def first(i, carry):
        base = pl.multiple_of((i + 1) * W, W)
        for p in range(planes):
            f = [raw[k, p, :, pl.ds(pl.multiple_of(base - W, W), W)] for k in range(19)]
            relax_and_store(0, f, p, base, 0)
        return carry

    lax.fori_loop(0, chunks, first, 0)
    flying = send(0, 0)

    for copy in mask_copies:
        copy.wait_recv()
    for zside, zsign in enumerate((1, -1)):
        offset = 0 if zsign == 1 else W + length
        block = mzh[ROUTES.index((0, zsign)) - 2]
        for p in range(planes):
            mask[p, :, offset : offset + W] = unpack(block, p, zsign == 1)
        for yside, ysign in enumerate((1, -1)):
            corner = mzh[ROUTES.index((ysign, zsign)) - 2]
            r = edge_row[ysign]
            for p in range(planes):
                moved = unpack(corner, p, zsign == 1)
                myh[yside, p : p + 1, offset : offset + W] = moved[r : r + 1, :]

    def flag(i, carry):
        base = pl.multiple_of((i + 1) * W, W)
        shifted = {}
        for q in range(planes):

            def cell(offset, q=q):
                return mask[q, :, pl.ds(pl.multiple_of(offset, W), W)]

            for cy in (0, 1, -1):

                def row(offset, q=q, cy=cy):
                    return myh[(1 - cy) // 2, q : q + 1, pl.ds(pl.multiple_of(offset, W), W)]

                for cz in (0, 1, -1):
                    shifted[q, cy, cz] = pull(cell, row, (0, cy, cz), base)
        for p in range(planes):
            word = jnp.zeros((across, W), jnp.int32)
            for k in range(1, 19):
                c = velocities[k]
                q = p - c[0]
                if 0 <= q < planes:
                    word = word | jnp.where(shifted[q, c[1], c[2]] > 0, 1 << k, 0)
            bits[p, :, pl.ds(pl.multiple_of(base - W, W), W)] = word
        return carry

    lax.fori_loop(0, chunks, flag, 0)

    all_copies = [mask_copies, flying]
    for step in range(STEPS - 1):
        source, into = step % 2, (step + 1) % 2
        arrive(step, source, flying)

        def middle(i, carry, step=step, source=source, into=into):
            base = pl.multiple_of((i + 1) * W, W)
            for p in range(planes):
                relax_and_store(step + 1, streamed(step, source, p, base), p, base, into)
            return carry

        lax.fori_loop(0, chunks, middle, 0)
        flying = send(step + 1, into)
        all_copies.append(flying)

    last = (STEPS - 1) % 2
    arrive(STEPS - 1, last, flying)

    def final(i, carry):
        base = pl.multiple_of((i + 1) * W, W)
        spot = pl.ds(pl.multiple_of(base - W, W), W)
        for p in range(planes):
            f = streamed(STEPS - 1, last, p, base)
            rho, jx, jy, jz = moments(f)[-4:]
            fluid = (1 - mask[p, :, pl.ds(base, W)]).astype(jnp.float32)
            den_ref[p, :, spot] = rho * fluid
            scale = fluid * (1.0 / reference_mach) / rho
            vel_ref[0, p, :, spot] = jx * scale
            vel_ref[1, p, :, spot] = jy * scale
            vel_ref[2, p, :, spot] = jz * scale
        return carry

    lax.fori_loop(0, chunks, final, 0)
    for group in all_copies:
        for copy in group:
            copy.wait_send()


def solution(mesh):
    gy, gz = mesh.shape["gy"], mesh.shape["gz"]

    def local(populations, solid_mask, body_force):
        planes, across, length = solid_mask.shape
        rows = len(Y_SET[1]) * planes
        wide = length + 2 * W
        return pl.pallas_call(
            functools.partial(kernel, gy, gz),
            out_shape=(
                jax.ShapeDtypeStruct((planes, across, length), jnp.float32),
                jax.ShapeDtypeStruct((3, planes, across, length), jnp.float32),
            ),
            in_specs=[
                pl.BlockSpec(memory_space=pl.ANY),
                pl.BlockSpec(memory_space=pl.ANY),
                pl.BlockSpec(memory_space=pltpu.SMEM),
            ],
            out_specs=(pl.BlockSpec(memory_space=pltpu.VMEM), pl.BlockSpec(memory_space=pltpu.VMEM)),
            scratch_shapes=[
                pltpu.VMEM((19, planes, across, length), jnp.float32),
                pltpu.VMEM((planes, across, wide), jnp.int32),
                pltpu.VMEM((planes, across, length), jnp.int32),
                pltpu.VMEM((2, 19, planes, across, wide), jnp.float32),
                pltpu.VMEM((STEPS, 2, rows, length), jnp.float32),
                pltpu.VMEM((STEPS, 2, rows, wide), jnp.float32),
                pltpu.VMEM((STEPS, 2, across, W), jnp.float32),
                pltpu.VMEM((STEPS, 6, across, W), jnp.float32),
                pltpu.VMEM((2, planes, length), jnp.int32),
                pltpu.VMEM((2, planes, wide), jnp.int32),
                pltpu.VMEM((2, across, W), jnp.int32),
                pltpu.VMEM((6, across, W), jnp.int32),
                pltpu.SemaphoreType.DMA((2,)),
                pltpu.SemaphoreType.DMA((STEPS + 1, len(ROUTES))),
                pltpu.SemaphoreType.DMA((STEPS + 1, len(ROUTES))),
            ],
            compiler_params=pltpu.CompilerParams(collective_id=0, has_side_effects=True),
        )(populations, solid_mask, body_force)

    return jax.shard_map(
        local,
        mesh=mesh,
        in_specs=(P(None, None, "gy", "gz"), P(None, "gy", "gz"), P()),
        out_specs=(P(None, "gy", "gz"), P(None, None, "gy", "gz")),
        check_vma=False,
    )
```

```python
import functools

import jax
import jax.numpy as jnp
from jax import lax
from jax.experimental import pallas as pl
from jax.experimental.pallas import tpu as pltpu
from jax.sharding import PartitionSpec as P

STEPS = 3
W = 128
UNROLL = 8
VMEM_LIMIT = 24 << 20

velocities = [
    (0, 0, 0),
    (1, 0, 0),
    (-1, 0, 0),
    (0, 1, 0),
    (0, -1, 0),
    (0, 0, 1),
    (0, 0, -1),
    (1, 1, 0),
    (-1, -1, 0),
    (1, -1, 0),
    (-1, 1, 0),
    (1, 0, 1),
    (-1, 0, -1),
    (1, 0, -1),
    (-1, 0, 1),
    (0, 1, 1),
    (0, -1, -1),
    (0, 1, -1),
    (0, -1, 1),
]
opposite = [0, 2, 1, 4, 3, 6, 5, 8, 7, 10, 9, 12, 11, 14, 13, 16, 15, 18, 17]
reference_mach = 0.05
Y_SET = {s: [k for k in range(19) if velocities[k][1] == s] for s in (1, -1)}
Z_SET = {s: [k for k in range(19) if velocities[k][2] == s] for s in (1, -1)}
ROUTES = [(1, 0), (-1, 0), (0, 1), (0, -1), (1, 1), (-1, 1), (1, -1), (-1, -1)]


def moments(f):
    s = [f[2 * a + 1] + f[2 * a + 2] for a in range(9)]
    d = [f[2 * a + 1] - f[2 * a + 2] for a in range(9)]
    axy, axz, ayz = s[3] + s[4], s[5] + s[6], s[7] + s[8]
    bxy, bxz, byz = s[3] - s[4], s[5] - s[6], s[7] - s[8]
    pxy, pxz, pyz = d[3] + d[4], d[5] + d[6], d[7] + d[8]
    qxy, qxz, qyz = d[3] - d[4], d[5] - d[6], d[7] - d[8]
    rho = (f[0] + s[0]) + (s[1] + s[2]) + ((axy + axz) + ayz)
    jx = d[0] + (pxy + pxz)
    jy = d[1] + (qxy + pyz)
    jz = d[2] + (qxz + qyz)
    return s, (axy, axz, ayz), (bxy, bxz, byz), (pxy, pxz, pyz), (qxy, qxz, qyz), rho, jx, jy, jz


def collide(f, force):
    s, (axy, axz, ayz), (bxy, bxz, byz), (pxy, pxz, pyz), (qxy, qxz, qyz), rho, jx, jy, jz = moments(f)
    inv = 1.0 / rho
    ux, uy, uz = jx * inv, jy * inv, jz * inv
    rxx, ryy, rzz = jx * ux, jy * uy, jz * uz
    third, ninth = rho * (1.0 / 3.0), rho * (1.0 / 9.0)
    e = 0.625
    exx = e * (s[0] + axy + axz - third - rxx)
    eyy = e * (s[1] + axy + ayz - third - ryy)
    ezz = e * (s[2] + axz + ayz - third - rzz)
    gxy = 0.5 * e * (bxy - jx * uy)
    gxz = 0.5 * e * (bxz - jx * uz)
    gyz = 0.5 * e * (byz - jy * uz)
    sq = (rxx + ryy + rzz) * (1.0 / 3.0)
    h = 0.65
    base = ninth + sq
    hxy = h * (axy - base + 0.5 * rzz)
    hxz = h * (axz - base + 0.5 * ryy)
    hyz = h * (ayz - base + 0.5 * rxx)
    t = 0.8
    jx3, jy3, jz3 = jx * (1.0 / 3.0), jy * (1.0 / 3.0), jz * (1.0 / 3.0)
    tpxy, tpxz, tpyz = t * (pxy - jx3), t * (pxz - jx3), t * (pyz - jy3)
    tqxy, tqxz, tqyz = t * (qxy - jy3), t * (qxz - jz3), t * (qyz - jz3)
    fx, fy, fz = force
    axis_w, edge_w = 3.0 / 18.0, 3.0 / 36.0
    even = [exx - hxy - hxz, eyy - hxy - hyz, ezz - hxz - hyz]
    odd = [-(tpxy + tpxz) - axis_w * fx, -(tqxy + tpyz) - axis_w * fy, -(tqxz + tqyz) - axis_w * fz]
    edges = (
        (hxy, gxy, tpxy, tqxy, fx, fy),
        (hxz, gxz, tpxz, tqxz, fx, fz),
        (hyz, gyz, tpyz, tqyz, fy, fz),
    )
    for hh, gg, tp, tq, fa, fb in edges:
        even += [0.5 * hh + gg, 0.5 * hh - gg]
        odd += [0.5 * (tp + tq) - edge_w * (fa + fb), 0.5 * (tp - tq) - edge_w * (fa - fb)]
    out = [f[0] + 2.0 * ((exx + eyy + ezz) - (hxy + hxz + hyz))]
    for a in range(9):
        out.append(f[2 * a + 1] - even[a] - odd[a])
        out.append(f[2 * a + 2] - even[a] + odd[a])
    return out


def kernel(gy, gz, pop_hbm, mask_hbm, force_ref, out_ref, raw, mask, bits, cells, ys, yh, zs, zh,
           mys, myh, mzs, mzh, load_sem, send_sem, recv_sem):
    planes, across, length = mask_hbm.shape
    chunks = length // W
    my, mz = lax.axis_index("gy"), lax.axis_index("gz")

    def peer(dy, dz):
        return {"gy": lax.rem(my + dy + gy, gy), "gz": lax.rem(mz + dz + gz, gz)}

    load_mask = pltpu.make_async_copy(mask_hbm, mask.at[:, :, W : W + length], load_sem.at[0])
    load_pop = [pltpu.make_async_copy(pop_hbm.at[:, p], raw.at[p], load_sem.at[1 + p]) for p in range(planes)]
    load_mask.start()
    for copy in load_pop:
        copy.start()
    barrier = pltpu.get_barrier_semaphore()
    for dy, dz in ROUTES:
        pl.semaphore_signal(barrier, inc=1, device_id=peer(dy, dz), device_id_type=pl.DeviceIdType.MESH)

    lane = lax.broadcasted_iota(jnp.int32, (across, W), 1)
    sub = lax.broadcasted_iota(jnp.int32, (across, W), 0)
    edge_row = {1: across - 1, -1: 0}

    def copies(number, rows_out, rows_in, packed_out, packed_in):
        result = []
        for i, (dy, dz) in enumerate(ROUTES):
            if dz == 0:
                side = (1 - dy) // 2
                source, target = rows_out.at[side], rows_in.at[side, :, W : W + length]
            else:
                source, target = packed_out.at[(1 - dz) // 2], packed_in.at[i - 2]
            result.append(
                pltpu.make_async_remote_copy(
                    src_ref=source,
                    dst_ref=target,
                    send_sem=send_sem.at[number, i],
                    recv_sem=recv_sem.at[number, i],
                    device_id=peer(dy, dz),
                    device_id_type=pl.DeviceIdType.MESH,
                )
            )
        return result

    def pack_columns(items, first, zero):
        packed = zero
        for j, block in enumerate(items):
            shift = (j if first else j + 1) % W
            moved = pltpu.roll(block, shift, 1) if shift else block
            packed = jnp.where(lane == j, moved, packed)
        return packed

    def unpack(block, j, last):
        shift = (W - 1 - j if last else W - j) % W
        return pltpu.roll(block, shift, 1) if shift else block

    def pull(cell, row, c, base):
        cy, cz = c[1], c[2]

        def at(offset):
            v = cell(offset)
            if cy:
                v = jnp.where(sub == edge_row[cy], row(offset), v)
            return v

        v = at(base)
        if cz == 1:
            v = pltpu.roll(jnp.where(lane == W - 1, at(base - W), v), 1, 1)
        elif cz == -1:
            v = pltpu.roll(jnp.where(lane == 0, at(base + W), v), W - 1, 1)
        if cy:
            v = pltpu.roll(v, 1 if cy == 1 else across - 1, 0)
        return v

    load_mask.wait()
    for side, sign in enumerate((1, -1)):
        for p in range(planes):
            r = edge_row[sign]
            mys[side, p : p + 1, :] = mask[p, r : r + 1, W : W + length]
        offset = length if sign == 1 else W
        mzs[side] = pack_columns(
            [mask[p, :, offset : offset + W] for p in range(planes)], sign == -1, jnp.zeros((across, W), jnp.int32)
        )
    pl.semaphore_wait(barrier, len(ROUTES))
    mask_copies = copies(0, mys, myh, mzs, mzh)
    for copy in mask_copies:
        copy.start()

    force = (force_ref[0], force_ref[1], force_ref[2])

    def relax_and_store(step, f, p, base, into):
        relaxed = collide(f, force)
        for k in range(19):
            cells[into, k, p, :, pl.ds(base, W)] = relaxed[k]
        start = pl.multiple_of(base - W, W)
        for side, sign in enumerate((1, -1)):
            r = edge_row[sign]
            for i, k in enumerate(Y_SET[sign]):
                ys[step, p, side, i : i + 1, pl.ds(start, W)] = relaxed[k][r : r + 1, :]

    def send(step, into, p):
        for side, sign in enumerate((1, -1)):
            offset = length if sign == 1 else W
            zs[step, p, side] = pack_columns(
                [cells[into, k, p, :, offset : offset + W] for k in Z_SET[sign]],
                sign == -1,
                jnp.zeros((across, W), jnp.float32),
            )
        out = copies(1 + step * planes + p, ys.at[step, p], yh.at[step, p], zs.at[step, p], zh.at[step, p])
        for copy in out:
            copy.start()
        return out

    def arrive(step, into, out, p):
        for copy in out:
            copy.wait_recv()
        for zsign in (1, -1):
            offset = 0 if zsign == 1 else W + length
            block = zh[step, p, ROUTES.index((0, zsign)) - 2]
            for i, k in enumerate(Z_SET[zsign]):
                cells[into, k, p, :, offset : offset + W] = unpack(block, i, zsign == 1)
            for yside, ysign in enumerate((1, -1)):
                corner = zh[step, p, ROUTES.index((ysign, zsign)) - 2]
                r = edge_row[ysign]
                k = velocities.index((0, ysign, zsign))
                moved = unpack(corner, Z_SET[zsign].index(k), zsign == 1)
                j = Y_SET[ysign].index(k)
                yh[step, p, yside, j : j + 1, offset : offset + W] = moved[r : r + 1, :]

    def streamed(step, into, p, base):
        flags = bits[p, :, pl.ds(pl.multiple_of(base - W, W), W)]
        f = []
        for k in range(19):
            c = velocities[k]
            here = cells[into, opposite[k], p, :, pl.ds(base, W)]
            q = p - c[0]
            if k == 0:
                moved = here
            elif q < 0 or q >= planes:
                f.append(here)
                continue
            else:

                def cell(offset, k=k, q=q):
                    return cells[into, k, q, :, pl.ds(pl.multiple_of(offset, W), W)]

                def row(offset, k=k, q=q, c=c):
                    j = Y_SET[c[1]].index(k)
                    return yh[step, q, (1 - c[1]) // 2, j : j + 1, pl.ds(pl.multiple_of(offset, W), W)]

                moved = pull(cell, row, c, base)
            f.append(moved if k == 0 else jnp.where((flags & (1 << k)) != 0, here, moved))
        return f

    unroll = max(u for u in (UNROLL, 4, 2, 1) if chunks % u == 0)

    def over_chunks(block):
        def group(i, carry):
            for n in range(unroll):
                block(pl.multiple_of((i * unroll + (n + 1)) * W, W))
            return carry

        lax.fori_loop(0, chunks // unroll, group, 0)

    flying = []
    for p in range(planes):
        load_pop[p].wait()

        def first(base, p=p):
            f = [raw[p, k, :, pl.ds(pl.multiple_of(base - W, W), W)] for k in range(19)]
            relax_and_store(0, f, p, base, 0)

        over_chunks(first)
        flying.append(send(0, 0, p))

    for copy in mask_copies:
        copy.wait_recv()
    for zside, zsign in enumerate((1, -1)):
        offset = 0 if zsign == 1 else W + length
        block = mzh[ROUTES.index((0, zsign)) - 2]
        for p in range(planes):
            mask[p, :, offset : offset + W] = unpack(block, p, zsign == 1)
        for yside, ysign in enumerate((1, -1)):
            corner = mzh[ROUTES.index((ysign, zsign)) - 2]
            r = edge_row[ysign]
            for p in range(planes):
                moved = unpack(corner, p, zsign == 1)
                myh[yside, p : p + 1, offset : offset + W] = moved[r : r + 1, :]

    def flag(i, carry):
        base = pl.multiple_of((i + 1) * W, W)
        shifted = {}
        for q in range(planes):

            def cell(offset, q=q):
                return mask[q, :, pl.ds(pl.multiple_of(offset, W), W)]

            for cy in (0, 1, -1):

                def row(offset, q=q, cy=cy):
                    return myh[(1 - cy) // 2, q : q + 1, pl.ds(pl.multiple_of(offset, W), W)]

                for cz in (0, 1, -1):
                    shifted[q, cy, cz] = pull(cell, row, (0, cy, cz), base)
        for p in range(planes):
            word = jnp.zeros((across, W), jnp.int32)
            for k in range(1, 19):
                c = velocities[k]
                q = p - c[0]
                if 0 <= q < planes:
                    word = word | jnp.where(shifted[q, c[1], c[2]] > 0, 1 << k, 0)
            bits[p, :, pl.ds(pl.multiple_of(base - W, W), W)] = word
        return carry

    lax.fori_loop(0, chunks, flag, 0)

    all_copies = [mask_copies] + flying
    for step in range(STEPS):
        source, into = step % 2, (step + 1) % 2
        started = []
        arrived = 0
        for p in range(planes):
            while arrived < min(p + 2, planes):
                arrive(step, source, flying[arrived], arrived)
                arrived += 1

            def middle(base, p=p, step=step, source=source, into=into):
                relax_and_store(step + 1, streamed(step, source, p, base), p, base, into)

            def final(base, p=p, step=step, source=source):
                spot = pl.ds(pl.multiple_of(base - W, W), W)
                rho, jx, jy, jz = moments(streamed(step, source, p, base))[-4:]
                fluid = (1 - mask[p, :, pl.ds(base, W)]).astype(jnp.float32)
                scale = fluid * (1.0 / reference_mach) / rho
                out_ref[0, p, :, spot] = rho * fluid
                out_ref[1, p, :, spot] = jx * scale
                out_ref[2, p, :, spot] = jy * scale
                out_ref[3, p, :, spot] = jz * scale

            if step < STEPS - 1:
                over_chunks(middle)
                started.append(send(step + 1, into, p))
            else:
                over_chunks(final)
        flying = started
        all_copies += flying
    for group in all_copies:
        for copy in group:
            copy.wait_send()


def hand_out(both_ref, den_hbm, vel_hbm, sem):
    den = pltpu.make_async_copy(both_ref.at[0], den_hbm, sem.at[0])
    vel = pltpu.make_async_copy(both_ref.at[pl.ds(1, 3)], vel_hbm, sem.at[1])
    vel.start()
    den.start()
    vel.wait()
    den.wait()


def solution(mesh):
    gy, gz = mesh.shape["gy"], mesh.shape["gz"]

    def local(populations, solid_mask, body_force):
        planes, across, length = solid_mask.shape
        rows = len(Y_SET[1])
        wide = length + 2 * W
        both = pl.pallas_call(
            functools.partial(kernel, gy, gz),
            out_shape=jax.ShapeDtypeStruct((4, planes, across, length), jnp.float32),
            in_specs=[
                pl.BlockSpec(memory_space=pltpu.HBM),
                pl.BlockSpec(memory_space=pltpu.HBM),
                pl.BlockSpec(memory_space=pltpu.SMEM),
            ],
            out_specs=pl.BlockSpec(memory_space=pltpu.VMEM),
            scratch_shapes=[
                pltpu.VMEM((planes, 19, across, length), jnp.float32),
                pltpu.VMEM((planes, across, wide), jnp.int32),
                pltpu.VMEM((planes, across, length), jnp.int32),
                pltpu.VMEM((2, 19, planes, across, wide), jnp.float32),
                pltpu.VMEM((STEPS, planes, 2, rows, length), jnp.float32),
                pltpu.VMEM((STEPS, planes, 2, rows, wide), jnp.float32),
                pltpu.VMEM((STEPS, planes, 2, across, W), jnp.float32),
                pltpu.VMEM((STEPS, planes, 6, across, W), jnp.float32),
                pltpu.VMEM((2, planes, length), jnp.int32),
                pltpu.VMEM((2, planes, wide), jnp.int32),
                pltpu.VMEM((2, across, W), jnp.int32),
                pltpu.VMEM((6, across, W), jnp.int32),
                pltpu.SemaphoreType.DMA((1 + planes,)),
                pltpu.SemaphoreType.DMA((STEPS * planes + 1, len(ROUTES))),
                pltpu.SemaphoreType.DMA((STEPS * planes + 1, len(ROUTES))),
            ],
            compiler_params=pltpu.CompilerParams(collective_id=0, has_side_effects=True, vmem_limit_bytes=VMEM_LIMIT),
        )(populations, solid_mask, body_force)
        return pl.pallas_call(
            hand_out,
            out_shape=(
                jax.ShapeDtypeStruct((planes, across, length), jnp.float32),
                jax.ShapeDtypeStruct((3, planes, across, length), jnp.float32),
            ),
            in_specs=[pl.BlockSpec(memory_space=pltpu.VMEM)],
            out_specs=(pl.BlockSpec(memory_space=pl.ANY), pl.BlockSpec(memory_space=pl.ANY)),
            scratch_shapes=[pltpu.SemaphoreType.DMA((2,))],
            compiler_params=pltpu.CompilerParams(vmem_limit_bytes=VMEM_LIMIT),
        )(both)

    return jax.shard_map(
        local,
        mesh=mesh,
        in_specs=(P(None, None, "gy", "gz"), P(None, "gy", "gz"), P()),
        out_specs=(P(None, "gy", "gz"), P(None, None, "gy", "gz")),
        check_vma=False,
    )
```
